256 devices in a mesh: req: 32 (over y, z), ctx: 8 (over x, core).
Axes of the slice: x: 4, y: 4, z: 8, core: 2. Of those that a mesh axis runs over, the one named last changes fastest.
Arguments:
- history: bfloat16 [196608, 1024], P(('req', 'ctx')), may hold values from -6 to 6
- block_owner: int32 [12288, 1], P(('req', 'ctx')), may hold values from 0 to 31; in each aligned block of 48 rows (0 to 47, 48 to 95, ...) at most 3 rows name the same one
- candidates: bfloat16 [32768, 1024], P(('req', 'ctx')), may hold values from -6 to 6
- w_kv: bfloat16 [1024, 2048], replicated, may hold values from -0.1875 to 0.1875
- w_qu: bfloat16 [1024, 2048], replicated, may hold values from -0.1875 to 0.1875
- w_out: bfloat16 [1024, 1024], replicated, may hold values from -0.1875 to 0.1875
Outputs:
- scored: bfloat16 [32768, 1024], P(('req', 'ctx'))
The draws below stay inside these ranges and needn't reach their ends.
Inputs may be any that keep to these rules, and one draw needn't show every extreme that they name: `block_owner`: each packed block belongs to one request; among the 48 blocks of one device at most 3 belong to the same request, and that most is reached on some device; every request owns at least one block.
All inputs are finite; a program needn't handle non-finite values.
Results may differ from the reference program's by a relative error of at most 0.0052.
Values may be sent and summed in bfloat16 or wider, within the bound.
A program may use at most 128 MiB of HBM per device.

```python
import math
import jax
import jax.numpy as jnp
import numpy as np
from jax import lax

D = 1024
HEAD = 128
BLK = 16
NB = 48
CAP = 3
CANDS = 1024
REQUESTS = 32
NBLOCKS = 12288
HIST = 196608
N_REQ = 32
N_CTX = 8


def block_levels(stream_key, shape, split, least, largest):
    def one(axis_at, shards_of):
        steps = jax.random.uniform(jax.random.fold_in(jax.random.fold_in(stream_key, 6), axis_at), (shards_of,), jnp.float32, least / len(split), largest / len(split))
        return jnp.repeat(jnp.exp(steps), shape[axis_at] // shards_of).reshape((-1,) + (1,) * (len(shape) - axis_at - 1))

    loudness = one(*split[0])
    for cut in split[1:]:
        loudness = loudness * one(*cut)
    return loudness


def shared_out(own_key, own, number, rows, number_of, top, reach, slope):
    order = jax.random.permutation(own_key, number_of)
    crowded, ordinary = load_shares(number_of, rows * top, reach, slope, True), load_shares(number_of, rows * top, reach, slope, False)
    places = jnp.arange(number_of)

    def named(lengths, rotation):
        used = int((lengths > 0).sum())
        fixed = max(1, used // 4)
        passed = fixed + (places - fixed + rotation * (used - fixed)) % max(1, number_of - fixed)
        return jnp.zeros((number_of,), jnp.int32).at[order[jnp.where(places < fixed, places, passed)]].set(jnp.asarray(lengths, jnp.int32))

    lengths = jnp.where(number % 4 == 0, named(crowded, number // 4), named(ordinary, number - number // 4 - 1))
    mixed = jax.random.permutation(jax.random.fold_in(own, 3), number_of)
    donor, receiver = mixed[0:number_of // 2 * 2:2], mixed[1:number_of // 2 * 2:2]
    room = jnp.minimum(lengths[donor] - 1, reach - lengths[receiver]) // 2
    room = jnp.where((donor == order[0]) | (receiver == order[0]) | (lengths[receiver] == 0), 0, jnp.maximum(room, 0))
    passed = jax.random.randint(jax.random.fold_in(own, 4), (number_of // 2,), 0, 1 << 20) % (room + 1)
    lengths = lengths.at[donor].add(-passed).at[receiver].add(passed)
    items = jnp.searchsorted(jnp.cumsum(lengths), jnp.arange(rows * top), side="right").astype(jnp.int32)
    listing = items.reshape(top, rows).T
    listing = listing[jax.random.permutation(jax.random.fold_in(own, 1), rows)]
    rotation = jax.random.randint(jax.random.fold_in(own, 2), (rows, 1), 0, top)
    return jnp.take_along_axis(listing, (jnp.arange(top)[None, :] + rotation) % top, axis=1)


def load_shares(number_of, total, bound, lean, full):
    portions = [(1 << 20) // math.isqrt(standing ** lean) + 1 for standing in range(1, number_of + 1)]
    largest = bound if full else min(bound, max(-(-total // number_of), total * portions[0] // sum(portions)))
    least = 1 if total - largest >= number_of - 1 else 0
    counts, surplus = [largest] + [least] * (number_of - 1), total - largest - least * (number_of - 1)
    while surplus > 0:
        free = [i for i in range(1, number_of) if counts[i] < largest] or [i for i in range(1, number_of) if counts[i] < bound]
        mass, remaining = sum([portions[i] for i in free]), surplus
        for i in free:
            more = min(bound - counts[i], max(1, remaining * portions[i] // mass), surplus)
            counts[i] = counts[i] + more
            surplus = surplus - more
    return np.array(counts)


def normal_values(own_key, shape, scale, limit, cuts=(), kind=jnp.bfloat16):
    values = jax.random.normal(own_key, shape, jnp.float32) * scale
    if len(cuts) > 0:
        values = block_levels(own_key, shape, cuts, -0.22, 0.18) * values
    return jnp.clip(values, min=-limit, max=limit).astype(kind)


def setup_inputs(seed: int = 0) -> dict:
    seeds = jax.random.split(jax.random.key(seed), 7)
    history = normal_values(seeds[0], (HIST, D), 1.0, 6.0, ((0, 256),))
    block_owner_keys = jax.random.split(jax.random.fold_in(seeds[1], 1), NBLOCKS // NB)
    block_owner_turns = jax.random.permutation(jax.random.fold_in(seeds[1], 3), NBLOCKS // NB)
    block_owner = jax.vmap(lambda own, number: shared_out(jax.random.fold_in(seeds[1], 2), own, number, NB, N_REQ, 1, CAP, 2))(block_owner_keys, block_owner_turns).reshape((NBLOCKS, 1))
    candidates = normal_values(seeds[2], (REQUESTS * CANDS, D), 1.0, 6.0, ((0, 256),))
    w_kv = normal_values(seeds[3], (D, 2 * D), D ** -0.5, 0.1875)
    w_qu = normal_values(seeds[4], (D, 2 * D), D ** -0.5, 0.1875)
    w_out = normal_values(seeds[5], (D, D), D ** -0.5, 0.1875)
    return {"history": history, "block_owner": block_owner, "candidates": candidates, "w_kv": w_kv, "w_qu": w_qu, "w_out": w_out}


key_span = 512

def attend(queries, keys_values):
    count, width = queries.shape
    heads = width // HEAD
    rows = keys_values.shape[0]
    span = key_span if rows % key_span == 0 else rows
    query = queries.astype(jnp.float32).reshape(count, heads, HEAD)
    pieces = keys_values.reshape(rows // span, span, 2, heads, HEAD)
    factor = HEAD ** (-0.5)

    def add_block(total, piece):
        keys = piece[:, 0].astype(jnp.float32)
        values = piece[:, 1].astype(jnp.float32)
        scores = jnp.einsum('qhd,khd->hqk', query, keys) * factor
        weights = jax.nn.silu(scores).astype(jnp.bfloat16).astype(jnp.float32)
        return (total + jnp.einsum('hqk,khd->qhd', weights, values), None)
    total, _ = lax.scan(add_block, jnp.zeros((count, heads, HEAD), jnp.float32), pieces)
    return total.reshape(count, width)

def reference(history, block_owner, candidates, w_kv, w_qu, w_out):
    devices = N_REQ * N_CTX
    raw = jnp.dot(history, w_kv, preferred_element_type=jnp.float32)
    keys_values = jnp.concatenate([jax.nn.silu(raw[:, :D]), raw[:, D:]], axis=1).astype(jnp.bfloat16)
    blocks = keys_values.reshape(devices, NB, BLK * 2 * D)
    owner = block_owner[:, 0].reshape(devices, NB)
    onehot = (owner[:, :, None] == jnp.arange(N_REQ, dtype=jnp.int32)[None, None, :]).astype(jnp.int32)
    rank = lax.optimization_barrier(jnp.sum((jnp.cumsum(onehot, axis=1) - onehot) * onehot, axis=2))
    slot = owner * CAP + rank
    projected = jnp.dot(candidates, w_qu, preferred_element_type=jnp.float32)
    queries = jax.nn.silu(projected[:, :D]).astype(jnp.bfloat16)
    gate = jax.nn.silu(projected[:, D:])

    def per_request(inputs):
        request, query = inputs
        wanted = request * CAP + jnp.arange(CAP, dtype=jnp.int32)
        hit = (slot[:, :, None] == wanted[None, None, :]).astype(jnp.int32)
        index = lax.optimization_barrier(jnp.sum(hit * jnp.arange(NB, dtype=jnp.int32)[None, :, None], axis=1)).astype(jnp.int32)
        valid = lax.optimization_barrier(jnp.sum(hit, axis=1))
        chosen = blocks[jnp.arange(devices, dtype=jnp.int32)[:, None], index]
        chosen = jnp.where(valid[:, :, None] > 0, chosen, jnp.zeros_like(chosen))
        return attend(query, chosen.reshape(devices * CAP * BLK, 2 * D))
    attended = lax.map(per_request, (jnp.arange(N_REQ, dtype=jnp.int32), queries.reshape(N_REQ, CANDS, D)))
    attended = attended.reshape(N_REQ * CANDS, D)
    mean = lax.optimization_barrier(jnp.mean(attended, axis=-1, keepdims=True))
    centred = attended - mean
    variance = lax.optimization_barrier(jnp.mean(centred * centred, axis=-1, keepdims=True))
    mixed = (centred * lax.rsqrt(variance + 1e-05) * gate).astype(jnp.bfloat16)
    result = candidates.astype(jnp.float32) + jnp.dot(mixed, w_out, preferred_element_type=jnp.float32)
    return result.astype(jnp.bfloat16)
```

```python
import functools

import jax
import jax.numpy as jnp
from jax import lax
from jax.experimental import pallas as pl
from jax.experimental.pallas import tpu as pltpu
from jax.sharding import PartitionSpec as P

HEAD = 128
REQ_CTX = ("req", "ctx")
NY, NZ, NX = 4, 8, 4
CAP = 3
MESH = pl.DeviceIdType.MESH


def silu(v):
    half = 0.5 * v
    return half + half * jnp.tanh(half)


def chunk_dz(i):
    return 4 + lax.div(i + 1, 2) * (1 - 2 * lax.rem(i, 2))


def layer_kernel(
    owner_ref, hist_ref, cand_ref, wkv_ref, wqu_ref, wout_ref, out_ref,
    hist, cand, wkv, wqu, wout,
    send, recv, queries, gate, keys, values, acc,
    pair_out, pair_in, cross_out, cross_in, own,
    load_sem, send_sem, recv_sem, qsend_sem, qrecv_sem,
    psend_sem, precv_sem, xsend_sem, xrecv_sem,
):
    req, ctx = lax.axis_index("req"), lax.axis_index("ctx")
    y, z = lax.div(req, NZ), lax.rem(req, NZ)
    x, core = lax.div(ctx, 2), lax.rem(ctx, 2)
    rows, width = hist.shape
    blocks = owner_ref.shape[0]
    events = rows // blocks
    unit = CAP * events
    group = NY * unit
    cands = cand.shape[0]
    heads = width // HEAD

    loads = []
    for k, (src, dst) in enumerate(
        ((hist_ref, hist), (cand_ref, cand), (wqu_ref, wqu), (wkv_ref, wkv), (wout_ref, wout))
    ):
        copy = pltpu.make_async_copy(src, dst, load_sem.at[k])
        copy.start()
        loads.append(copy)

    barrier = pltpu.get_barrier_semaphore()
    for d in range(1, NY * NZ):
        pl.semaphore_signal(
            barrier, inc=1, device_id={"req": lax.rem(req + d, NY * NZ)}, device_id_type=MESH
        )
    for d in range(1, 2 * NX):
        pl.semaphore_signal(
            barrier, inc=1, device_id={"ctx": lax.rem(ctx + d, 2 * NX)}, device_id_type=MESH
        )

    owner = owner_ref[...].astype(jnp.float32)
    block_of = lax.div(lax.broadcasted_iota(jnp.int32, (blocks, rows), 1), events)
    earlier = lax.broadcasted_iota(jnp.int32, (blocks, rows), 0)
    owner_row = jnp.sum(jnp.where(earlier == block_of, owner, 0.0), axis=0, keepdims=True)
    same = jnp.logical_and(owner == owner_row, earlier < block_of)
    rank = jnp.sum(jnp.where(same, 1.0, 0.0), axis=0, keepdims=True)
    event = lax.rem(lax.broadcasted_iota(jnp.int32, (1, rows), 1), events)
    place = owner_row.astype(jnp.int32) * unit + rank.astype(jnp.int32) * events + event

    pl.semaphore_wait(barrier, NY * NZ + 2 * NX - 2)
    loads[0].wait()

    def exchange(i, j):
        to_y = lax.rem(y + j, NY)
        to_z = lax.rem(z + chunk_dz(i), NZ)
        spot = i * NY + j
        return pltpu.make_async_remote_copy(
            src_ref=send.at[pl.ds(pl.multiple_of(spot * unit, unit), unit)],
            dst_ref=recv.at[pl.ds(pl.multiple_of(spot * unit, unit), unit)],
            send_sem=send_sem.at[spot],
            recv_sem=recv_sem.at[spot],
            device_id={"req": to_y * NZ + to_z},
            device_id_type=MESH,
        )

    line = lax.broadcasted_iota(jnp.int32, (group, 1), 0)
    turn = sum(jnp.where(line >= unit * k, 1, 0) for k in range(1, NY))
    inside = line - turn * unit

    def pack(i):
        to_z = lax.rem(z + chunk_dz(i), NZ)
        target = (lax.rem(y + turn, NY) * NZ + to_z) * unit + inside
        placing = jnp.where(target == place, 1.0, 0.0).astype(jnp.bfloat16)
        return jnp.dot(placing, hist[...], preferred_element_type=jnp.float32).astype(jnp.bfloat16)

    last = NZ - 1

    @pl.loop(0, last)
    def _(i):
        send[pl.ds(pl.multiple_of(i * group, group), group), :] = pack(i)
        for j in range(NY):
            exchange(i, j).start()

    made = pack(last)
    recv[last * group : last * group + unit, :] = made[:unit]
    send[last * group + unit : (last + 1) * group, :] = made[unit:]
    for j in range(1, NY):
        exchange(last, j).start()

    loads[1].wait()
    loads[2].wait()
    mine = pl.ds(pl.multiple_of(ctx * cands, cands), cands)
    queries[mine, :] = silu(
        jnp.dot(cand[...], wqu[:, :width], preferred_element_type=jnp.float32)
    ).astype(jnp.bfloat16)

    def query_copy(d):
        return pltpu.make_async_remote_copy(
            src_ref=queries.at[mine],
            dst_ref=queries.at[mine],
            send_sem=qsend_sem.at[d],
            recv_sem=qrecv_sem.at[d],
            device_id={"ctx": lax.rem(ctx + d, 2 * NX)},
            device_id_type=MESH,
        )

    for d in range(1, 2 * NX):
        query_copy(d).start()
    gate[...] = silu(jnp.dot(cand[...], wqu[:, width:], preferred_element_type=jnp.float32))
    acc[...] = jnp.zeros_like(acc)
    loads[3].wait()

    def arrive(i):
        for j in range(NY):
            if j == 0:
                @pl.when(i < last)
                def _():
                    exchange(i, j).wait_recv()
            else:
                exchange(i, j).wait_recv()

    def project(i):
        events_in = recv[pl.ds(pl.multiple_of(i * group, group), group), :]
        keys[...] = silu(
            jnp.dot(events_in, wkv[:, :width], preferred_element_type=jnp.float32)
        ).astype(jnp.bfloat16)
        values[...] = jnp.dot(
            events_in, wkv[:, width:], preferred_element_type=jnp.float32
        ).astype(jnp.bfloat16)

    span = 2 * cands
    factor = 0.5 * HEAD ** (-0.5)

    def attend(at):
        here = pl.ds(pl.multiple_of(at * span, span), span)
        for h in range(heads):
            cols = slice(h * HEAD, (h + 1) * HEAD)
            scores = lax.dot_general(
                queries[here, cols], keys[:, cols], (((1,), (1,)), ((), ())),
                preferred_element_type=jnp.float32,
            )
            half = scores * factor
            weight = (half + half * jnp.tanh(half)).astype(jnp.bfloat16)
            acc[here, cols] += jnp.dot(
                weight, values[:, cols], preferred_element_type=jnp.float32
            )

    arrive(0)
    project(0)
    for d in range(1, 2 * NX):
        query_copy(d).wait_recv()

    @pl.loop(0, NX)
    def _(at):
        attend(at)

    @pl.loop(1, last)
    def _(i):
        arrive(i)
        project(i)

        @pl.loop(0, NX)
        def _(at):
            attend(at)

    arrive(last)
    project(last)

    def chip_at(i):
        return lax.rem(x + 2 + lax.div(i * (i + 1), 2), NX)

    def pair_copy(i):
        return pltpu.make_async_remote_copy(
            src_ref=pair_out.at[i],
            dst_ref=pair_in.at[i],
            send_sem=psend_sem.at[i],
            recv_sem=precv_sem.at[i],
            device_id={"ctx": 2 * x + 1 - core},
            device_id_type=MESH,
        )

    def cross_copy(i):
        return pltpu.make_async_remote_copy(
            src_ref=cross_out.at[i],
            dst_ref=cross_in.at[i],
            send_sem=xsend_sem.at[i],
            recv_sem=xrecv_sem.at[i],
            device_id={"ctx": 2 * chip_at(i) + core},
            device_id_type=MESH,
        )

    def part_of(i, which):
        at = 2 * chip_at(i) + which
        return acc[pl.ds(pl.multiple_of(at * cands, cands), cands), :]

    @pl.loop(0, NX)
    def _(i):
        attend(chip_at(i))
        pair_out[i] = part_of(i, 1 - core).astype(jnp.bfloat16)
        pair_copy(i).start()

    @pl.loop(0, NX - 1)
    def _(i):
        pair_copy(i).wait_recv()
        cross_out[i] = (part_of(i, core) + pair_in[i].astype(jnp.float32)).astype(jnp.bfloat16)
        cross_copy(i).start()

    pair_copy(NX - 1).wait_recv()
    own[...] = part_of(NX - 1, core) + pair_in[NX - 1].astype(jnp.float32)
    loads[4].wait()
    for i in (1, 2, 0):
        cross_copy(i).wait_recv()
    attended = own[...] + cross_in[0].astype(jnp.float32)
    attended = attended + cross_in[1].astype(jnp.float32) + cross_in[2].astype(jnp.float32)
    mean = jnp.mean(attended, axis=-1, keepdims=True)
    centred = attended - mean
    variance = jnp.mean(centred * centred, axis=-1, keepdims=True)
    mixed = (centred * lax.rsqrt(variance + 1e-05) * gate[...]).astype(jnp.bfloat16)
    result = cand[...].astype(jnp.float32) + jnp.dot(
        mixed, wout[...], preferred_element_type=jnp.float32
    )
    out_ref[...] = result.astype(jnp.bfloat16)

    @pl.loop(0, last)
    def _(i):
        for j in range(NY):
            exchange(i, j).wait_send()

    for j in range(1, NY):
        exchange(last, j).wait_send()
    for d in range(1, 2 * NX):
        query_copy(d).wait_send()
    for i in range(NX):
        pair_copy(i).wait_send()
    for i in range(NX - 1):
        cross_copy(i).wait_send()


def on_device(history, block_owner, candidates, w_kv, w_qu, w_out):
    rows, width = history.shape
    events = rows // block_owner.shape[0]
    cands = candidates.shape[0]
    group = NY * CAP * events
    total = NZ * group
    count = NY * NZ
    bf16, f32 = jnp.bfloat16, jnp.float32
    dma = pltpu.SemaphoreType.DMA
    anywhere = pl.BlockSpec(memory_space=pl.ANY)
    vmem = pl.BlockSpec(memory_space=pltpu.VMEM)
    return pl.pallas_call(
        layer_kernel,
        out_shape=jax.ShapeDtypeStruct((cands, width), bf16),
        in_specs=[vmem] + [anywhere] * 5,
        out_specs=vmem,
        scratch_shapes=[
            pltpu.VMEM((rows, width), bf16),
            pltpu.VMEM((cands, width), bf16),
            pltpu.VMEM((width, 2 * width), bf16),
            pltpu.VMEM((width, 2 * width), bf16),
            pltpu.VMEM((width, width), bf16),
            pltpu.VMEM((total, width), bf16),
            pltpu.VMEM((total, width), bf16),
            pltpu.VMEM((2 * NX * cands, width), bf16),
            pltpu.VMEM((cands, width), f32),
            pltpu.VMEM((group, width), bf16),
            pltpu.VMEM((group, width), bf16),
            pltpu.VMEM((2 * NX * cands, width), f32),
            pltpu.VMEM((NX, cands, width), bf16),
            pltpu.VMEM((NX, cands, width), bf16),
            pltpu.VMEM((NX - 1, cands, width), bf16),
            pltpu.VMEM((NX - 1, cands, width), bf16),
            pltpu.VMEM((cands, width), f32),
            dma((5,)),
            dma((count,)),
            dma((count,)),
            dma((2 * NX,)),
            dma((2 * NX,)),
            dma((NX,)),
            dma((NX,)),
            dma((NX - 1,)),
            dma((NX - 1,)),
        ],
        compiler_params=pltpu.CompilerParams(
            collective_id=0, has_side_effects=True, vmem_limit_bytes=60 * 2**20
        ),
    )(block_owner, history, candidates, w_kv, w_qu, w_out)


def solution(mesh):
    in_specs = (P(REQ_CTX, None), P(REQ_CTX, None), P(REQ_CTX, None), P(), P(), P())
    return jax.shard_map(
        on_device, mesh=mesh, in_specs=in_specs, out_specs=P(REQ_CTX, None), check_vma=False
    )
```

```python
import functools

import jax
import jax.numpy as jnp
from jax import lax
from jax.experimental import pallas as pl
from jax.experimental.pallas import tpu as pltpu
from jax.sharding import PartitionSpec as P

HEAD = 128
REQ_CTX = ("req", "ctx")
NY, NZ, NX = 4, 8, 4
CAP = 3
MESH = pl.DeviceIdType.MESH


def silu(v):
    half = 0.5 * v
    return half + half * jnp.tanh(half)


def chunk_dz(i):
    return lax.rem(NZ + lax.div(i + 1, 2) * (2 * lax.rem(i, 2) - 1), NZ)


def layer_kernel(
    owner_ref, hist_ref, cand_ref, wkv_ref, wqu_ref, wout_ref, out_ref,
    owners, hist, cand, wkv, wqu, wout,
    send, recv, queries, gate, keys, values, acc,
    pair_out, pair_in, cross_out, cross_in, own,
    load_sem, send_sem, recv_sem, qsend_sem, qrecv_sem,
    psend_sem, precv_sem, xsend_sem, xrecv_sem,
):
    req, ctx = lax.axis_index("req"), lax.axis_index("ctx")
    y, z = lax.div(req, NZ), lax.rem(req, NZ)
    x, core = lax.div(ctx, 2), lax.rem(ctx, 2)
    rows, width = hist.shape
    blocks = owner_ref.shape[1]
    events = rows // blocks
    unit = CAP * events
    group = NY * unit
    cands = cand.shape[0]
    heads = width // HEAD

    loads = []
    for k, (src, dst) in enumerate(
        (
            (owner_ref, owners), (hist_ref, hist), (cand_ref, cand),
            (wqu_ref, wqu), (wkv_ref, wkv), (wout_ref, wout),
        )
    ):
        copy = pltpu.make_async_copy(src, dst, load_sem.at[k])
        copy.start()
        loads.append(copy)

    barrier = pltpu.get_barrier_semaphore()
    for d in range(1, NY * NZ):
        pl.semaphore_signal(
            barrier, inc=1, device_id={"req": lax.rem(req + d, NY * NZ)}, device_id_type=MESH
        )
    for d in range(1, 2 * NX):
        pl.semaphore_signal(
            barrier, inc=1, device_id={"ctx": lax.rem(ctx + d, 2 * NX)}, device_id_type=MESH
        )

    loads[0].wait()
    spot = lax.broadcasted_iota(jnp.int32, (blocks, blocks), 0)
    diagonal = spot == lax.broadcasted_iota(jnp.int32, (blocks, blocks), 1)
    listed = owners[...].astype(jnp.float32)
    owner = jnp.sum(jnp.where(diagonal, listed, 0.0), axis=1, keepdims=True)
    block_of = lax.div(lax.broadcasted_iota(jnp.int32, (blocks, rows), 1), events)
    earlier = lax.broadcasted_iota(jnp.int32, (blocks, rows), 0)
    owner_row = jnp.sum(jnp.where(earlier == block_of, owner, 0.0), axis=0, keepdims=True)
    same = jnp.logical_and(owner == owner_row, earlier < block_of)
    rank = jnp.sum(jnp.where(same, 1.0, 0.0), axis=0, keepdims=True)
    event = lax.rem(lax.broadcasted_iota(jnp.int32, (1, rows), 1), events)
    place = owner_row.astype(jnp.int32) * unit + rank.astype(jnp.int32) * events + event

    loads[1].wait()

    def exchange(i, j):
        to_y = lax.rem(y + j, NY)
        to_z = lax.rem(z + chunk_dz(i), NZ)
        spot = i * NY + j
        return pltpu.make_async_remote_copy(
            src_ref=send.at[pl.ds(pl.multiple_of(spot * unit, unit), unit)],
            dst_ref=recv.at[pl.ds(pl.multiple_of(spot * unit, unit), unit)],
            send_sem=send_sem.at[spot],
            recv_sem=recv_sem.at[spot],
            device_id={"req": to_y * NZ + to_z},
            device_id_type=MESH,
        )

    line = lax.broadcasted_iota(jnp.int32, (group, 1), 0)
    turn = sum(jnp.where(line >= unit * k, 1, 0) for k in range(1, NY))
    inside = line - turn * unit

    def pack(i):
        to_z = lax.rem(z + chunk_dz(i), NZ)
        target = (lax.rem(y + turn, NY) * NZ + to_z) * unit + inside
        placing = jnp.where(target == place, 1.0, 0.0).astype(jnp.bfloat16)
        return jnp.dot(placing, hist[...], preferred_element_type=jnp.float32).astype(jnp.bfloat16)

    last, early = NZ - 1, 3
    made = pack(0)
    recv[:unit, :] = made[:unit]
    send[unit:group, :] = made[unit:]

    @pl.loop(1, early)
    def _(i):
        send[pl.ds(pl.multiple_of(i * group, group), group), :] = pack(i)

    pl.semaphore_wait(barrier, NY * NZ + 2 * NX - 2)
    for i in range(1, early):
        for j in range(NY):
            exchange(i, j).start()
    for j in range(1, NY):
        exchange(0, j).start()

    loads[2].wait()
    loads[3].wait()
    mine = pl.ds(pl.multiple_of(ctx * cands, cands), cands)
    queries[mine, :] = silu(
        jnp.dot(cand[...], wqu[:, :width], preferred_element_type=jnp.float32)
    ).astype(jnp.bfloat16)

    def query_copy(d):
        return pltpu.make_async_remote_copy(
            src_ref=queries.at[mine],
            dst_ref=queries.at[mine],
            send_sem=qsend_sem.at[d],
            recv_sem=qrecv_sem.at[d],
            device_id={"ctx": lax.rem(ctx + d, 2 * NX)},
            device_id_type=MESH,
        )

    for d in range(1, 2 * NX):
        query_copy(d).start()

    @pl.loop(early, NZ)
    def _(i):
        send[pl.ds(pl.multiple_of(i * group, group), group), :] = pack(i)
        for j in range(NY):
            exchange(i, j).start()

    gate[...] = silu(jnp.dot(cand[...], wqu[:, width:], preferred_element_type=jnp.float32))
    acc[...] = jnp.zeros_like(acc)
    loads[4].wait()

    def arrive(i):
        for j in range(NY):
            exchange(i, j).wait_recv()

    def project(i):
        events_in = recv[pl.ds(pl.multiple_of(i * group, group), group), :]
        keys[...] = silu(
            jnp.dot(events_in, wkv[:, :width], preferred_element_type=jnp.float32)
        ).astype(jnp.bfloat16)
        values[...] = jnp.dot(
            events_in, wkv[:, width:], preferred_element_type=jnp.float32
        ).astype(jnp.bfloat16)

    span = 2 * cands
    factor = 0.5 * HEAD ** (-0.5)

    def attend(at):
        here = pl.ds(pl.multiple_of(at * span, span), span)
        for h in range(heads):
            cols = slice(h * HEAD, (h + 1) * HEAD)
            scores = lax.dot_general(
                queries[here, cols], keys[:, cols], (((1,), (1,)), ((), ())),
                preferred_element_type=jnp.float32,
            )
            half = scores * factor
            weight = (half + half * jnp.tanh(half)).astype(jnp.bfloat16)
            acc[here, cols] += jnp.dot(
                weight, values[:, cols], preferred_element_type=jnp.float32
            )

    for j in range(1, NY):
        exchange(0, j).wait_recv()
    project(0)
    for d in range(1, 2 * NX):
        query_copy(d).wait_recv()

    @pl.loop(0, NX)
    def _(at):
        attend(at)

    @pl.loop(1, last)
    def _(i):
        arrive(i)
        project(i)

        @pl.loop(0, NX)
        def _(at):
            attend(at)

    arrive(last)
    project(last)

    def chip_at(i):
        return lax.rem(x + 2 + lax.div(i * (i + 1), 2), NX)

    def pair_copy(i):
        return pltpu.make_async_remote_copy(
            src_ref=pair_out.at[i],
            dst_ref=pair_in.at[i],
            send_sem=psend_sem.at[i],
            recv_sem=precv_sem.at[i],
            device_id={"ctx": 2 * x + 1 - core},
            device_id_type=MESH,
        )

    def cross_copy(i):
        return pltpu.make_async_remote_copy(
            src_ref=cross_out.at[i],
            dst_ref=cross_in.at[i],
            send_sem=xsend_sem.at[i],
            recv_sem=xrecv_sem.at[i],
            device_id={"ctx": 2 * chip_at(i) + core},
            device_id_type=MESH,
        )

    def part_of(i, which):
        at = 2 * chip_at(i) + which
        return acc[pl.ds(pl.multiple_of(at * cands, cands), cands), :]

    def cross(i):
        pair_copy(i).wait_recv()
        cross_out[i] = (part_of(i, core) + pair_in[i].astype(jnp.float32)).astype(jnp.bfloat16)
        cross_copy(i).start()

    @pl.loop(0, NX)
    def _(i):
        attend(chip_at(i))
        pair_out[i] = part_of(i, 1 - core).astype(jnp.bfloat16)
        pair_copy(i).start()

        @pl.when(i > 0)
        def _():
            cross(i - 1)

    pair_copy(NX - 1).wait_recv()
    own[...] = part_of(NX - 1, core) + pair_in[NX - 1].astype(jnp.float32)
    loads[5].wait()
    for i in (1, 2, 0):
        cross_copy(i).wait_recv()
    attended = own[...] + cross_in[0].astype(jnp.float32)
    attended = attended + cross_in[1].astype(jnp.float32) + cross_in[2].astype(jnp.float32)
    mean = jnp.mean(attended, axis=-1, keepdims=True)
    centred = attended - mean
    variance = jnp.mean(centred * centred, axis=-1, keepdims=True)
    mixed = (centred * lax.rsqrt(variance + 1e-05) * gate[...]).astype(jnp.bfloat16)
    result = cand[...].astype(jnp.float32) + jnp.dot(
        mixed, wout[...], preferred_element_type=jnp.float32
    )
    out_ref[...] = result.astype(jnp.bfloat16)

    for j in range(1, NY):
        exchange(0, j).wait_send()

    @pl.loop(1, NZ)
    def _(i):
        for j in range(NY):
            exchange(i, j).wait_send()

    for d in range(1, 2 * NX):
        query_copy(d).wait_send()
    for i in range(NX):
        pair_copy(i).wait_send()
    for i in range(NX - 1):
        cross_copy(i).wait_send()


def on_device(history, block_owner, candidates, w_kv, w_qu, w_out):
    rows, width = history.shape
    blocks = block_owner.shape[0]
    events = rows // blocks
    cands = candidates.shape[0]
    group = NY * CAP * events
    total = NZ * group
    count = NY * NZ
    bf16, f32 = jnp.bfloat16, jnp.float32
    dma = pltpu.SemaphoreType.DMA
    anywhere = pl.BlockSpec(memory_space=pl.ANY)
    vmem = pl.BlockSpec(memory_space=pltpu.VMEM)
    return pl.pallas_call(
        layer_kernel,
        out_shape=jax.ShapeDtypeStruct((cands, width), bf16),
        in_specs=[anywhere] * 6,
        out_specs=vmem,
        scratch_shapes=[
            pltpu.VMEM((1, blocks), jnp.int32),
            pltpu.VMEM((rows, width), bf16),
            pltpu.VMEM((cands, width), bf16),
            pltpu.VMEM((width, 2 * width), bf16),
            pltpu.VMEM((width, 2 * width), bf16),
            pltpu.VMEM((width, width), bf16),
            pltpu.VMEM((total, width), bf16),
            pltpu.VMEM((total, width), bf16),
            pltpu.VMEM((2 * NX * cands, width), bf16),
            pltpu.VMEM((cands, width), f32),
            pltpu.VMEM((group, width), bf16),
            pltpu.VMEM((group, width), bf16),
            pltpu.VMEM((2 * NX * cands, width), f32),
            pltpu.VMEM((NX, cands, width), bf16),
            pltpu.VMEM((NX, cands, width), bf16),
            pltpu.VMEM((NX - 1, cands, width), bf16),
            pltpu.VMEM((NX - 1, cands, width), bf16),
            pltpu.VMEM((cands, width), f32),
            dma((6,)),
            dma((count,)),
            dma((count,)),
            dma((2 * NX,)),
            dma((2 * NX,)),
            dma((NX,)),
            dma((NX,)),
            dma((NX - 1,)),
            dma((NX - 1,)),
        ],
        compiler_params=pltpu.CompilerParams(
            collective_id=0, has_side_effects=True, vmem_limit_bytes=60 * 2**20
        ),
    )(block_owner.reshape(1, blocks), history, candidates, w_kv, w_qu, w_out)


def solution(mesh):
    in_specs = (P(REQ_CTX, None), P(REQ_CTX, None), P(REQ_CTX, None), P(), P(), P())
    return jax.shard_map(
        on_device, mesh=mesh, in_specs=in_specs, out_specs=P(REQ_CTX, None), check_vma=False
    )
```

```python
import functools

import jax
import jax.numpy as jnp
from jax import lax
from jax.experimental import pallas as pl
from jax.experimental.pallas import tpu as pltpu
from jax.sharding import PartitionSpec as P

HEAD = 128
REQ_CTX = ("req", "ctx")
NY, NZ, NX = 4, 8, 4
CAP = 3
MESH = pl.DeviceIdType.MESH


def silu(v):
    half = 0.5 * v
    return half + half * jnp.tanh(half)


def chunk_dz(i):
    return lax.rem(NZ + lax.div(i + 1, 2) * (2 * lax.rem(i, 2) - 1), NZ)


def layer_kernel(
    owner_ref, hist_ref, cand_ref, wkv_ref, wqu_ref, wout_ref, out_ref,
    owners, hist, cand, wkv, wqu, wout,
    send, recv, queries, gate, keys, values, acc,
    pair_out, pair_in, cross_out, cross_in, own,
    load_sem, send_sem, recv_sem, qsend_sem, qrecv_sem,
    psend_sem, precv_sem, xsend_sem, xrecv_sem,
):
    req, ctx = lax.axis_index("req"), lax.axis_index("ctx")
    y, z = lax.div(req, NZ), lax.rem(req, NZ)
    x, core = lax.div(ctx, 2), lax.rem(ctx, 2)
    rows, width = hist.shape
    blocks = owner_ref.shape[1]
    events = rows // blocks
    unit = CAP * events
    group = NY * unit
    cands = cand.shape[0]
    heads = width // HEAD

    loads = []
    for k, (src, dst) in enumerate(
        (
            (owner_ref, owners), (hist_ref, hist), (cand_ref, cand),
            (wqu_ref, wqu), (wkv_ref, wkv), (wout_ref, wout),
        )
    ):
        loads.append(pltpu.make_async_copy(src, dst, load_sem.at[k]))
    loads[0].start()
    loads[1].start()

    barrier = pltpu.get_barrier_semaphore()
    for d in range(1, NY * NZ):
        pl.semaphore_signal(
            barrier, inc=1, device_id={"req": lax.rem(req + d, NY * NZ)}, device_id_type=MESH
        )
    for d in range(1, 2 * NX):
        pl.semaphore_signal(
            barrier, inc=1, device_id={"ctx": lax.rem(ctx + d, 2 * NX)}, device_id_type=MESH
        )

    loads[0].wait()
    spot = lax.broadcasted_iota(jnp.int32, (blocks, blocks), 0)
    diagonal = spot == lax.broadcasted_iota(jnp.int32, (blocks, blocks), 1)
    listed = owners[...].astype(jnp.float32)
    owner = jnp.sum(jnp.where(diagonal, listed, 0.0), axis=1, keepdims=True)
    block_of = lax.div(lax.broadcasted_iota(jnp.int32, (blocks, rows), 1), events)
    earlier = lax.broadcasted_iota(jnp.int32, (blocks, rows), 0)
    owner_row = jnp.sum(jnp.where(earlier == block_of, owner, 0.0), axis=0, keepdims=True)
    same = jnp.logical_and(owner == owner_row, earlier < block_of)
    rank = jnp.sum(jnp.where(same, 1.0, 0.0), axis=0, keepdims=True)
    event = lax.rem(lax.broadcasted_iota(jnp.int32, (1, rows), 1), events)
    place = owner_row.astype(jnp.int32) * unit + rank.astype(jnp.int32) * events + event

    loads[1].wait()
    for copy in loads[2:]:
        copy.start()

    def exchange(i, j):
        to_y = lax.rem(y + j, NY)
        to_z = lax.rem(z + chunk_dz(i), NZ)
        spot = i * NY + j
        return pltpu.make_async_remote_copy(
            src_ref=send.at[pl.ds(pl.multiple_of(spot * unit, unit), unit)],
            dst_ref=recv.at[pl.ds(pl.multiple_of(spot * unit, unit), unit)],
            send_sem=send_sem.at[spot],
            recv_sem=recv_sem.at[spot],
            device_id={"req": to_y * NZ + to_z},
            device_id_type=MESH,
        )

    line = lax.broadcasted_iota(jnp.int32, (group, 1), 0)
    turn = sum(jnp.where(line >= unit * k, 1, 0) for k in range(1, NY))
    inside = line - turn * unit

    def pack(i):
        to_z = lax.rem(z + chunk_dz(i), NZ)
        target = (lax.rem(y + turn, NY) * NZ + to_z) * unit + inside
        placing = jnp.where(target == place, 1.0, 0.0).astype(jnp.bfloat16)
        return jnp.dot(placing, hist[...], preferred_element_type=jnp.float32).astype(jnp.bfloat16)

    last, early = NZ - 1, 3
    turns = (1, 3, 0, 2)

    def fill(i):
        send[pl.ds(pl.multiple_of(i * group, group), group), :] = pack(i)

    @pl.loop(1, early)
    def _(i):
        fill(i)

    pl.semaphore_wait(barrier, NY * NZ + 2 * NX - 2)
    for j in turns:
        for i in range(1, early):
            exchange(i, j).start()
    made = pack(0)
    recv[:unit, :] = made[:unit]
    send[unit:group, :] = made[unit:]
    for j in range(1, NY):
        exchange(0, j).start()

    loads[2].wait()
    loads[3].wait()
    mine = pl.ds(pl.multiple_of(ctx * cands, cands), cands)
    queries[mine, :] = silu(
        jnp.dot(cand[...], wqu[:, :width], preferred_element_type=jnp.float32)
    ).astype(jnp.bfloat16)

    def query_copy(d):
        return pltpu.make_async_remote_copy(
            src_ref=queries.at[mine],
            dst_ref=queries.at[mine],
            send_sem=qsend_sem.at[d],
            recv_sem=qrecv_sem.at[d],
            device_id={"ctx": lax.rem(ctx + d, 2 * NX)},
            device_id_type=MESH,
        )

    for d in range(1, 2 * NX):
        query_copy(d).start()

    @pl.loop(0, (last - early) // 2)
    def _(p):
        first = early + 2 * p

        @pl.loop(first, first + 2)
        def _(i):
            fill(i)

        for j in turns:
            exchange(first, j).start()
            exchange(first + 1, j).start()

    fill(last)
    for j in turns:
        exchange(last, j).start()

    gate[...] = silu(jnp.dot(cand[...], wqu[:, width:], preferred_element_type=jnp.float32))
    acc[...] = jnp.zeros_like(acc)
    loads[4].wait()

    def arrive(i):
        for j in range(NY):
            exchange(i, j).wait_recv()

    def project(i):
        events_in = recv[pl.ds(pl.multiple_of(i * group, group), group), :]
        keys[...] = silu(
            jnp.dot(events_in, wkv[:, :width], preferred_element_type=jnp.float32)
        ).astype(jnp.bfloat16)
        values[...] = jnp.dot(
            events_in, wkv[:, width:], preferred_element_type=jnp.float32
        ).astype(jnp.bfloat16)

    span = 2 * cands
    factor = 0.5 * HEAD ** (-0.5)

    def attend(at):
        here = pl.ds(pl.multiple_of(at * span, span), span)
        for h in range(heads):
            cols = slice(h * HEAD, (h + 1) * HEAD)
            scores = lax.dot_general(
                queries[here, cols], keys[:, cols], (((1,), (1,)), ((), ())),
                preferred_element_type=jnp.float32,
            )
            half = scores * factor
            weight = (half + half * jnp.tanh(half)).astype(jnp.bfloat16)
            acc[here, cols] += jnp.dot(
                weight, values[:, cols], preferred_element_type=jnp.float32
            )

    for j in range(1, NY):
        exchange(0, j).wait_recv()
    project(0)
    for d in range(1, 2 * NX):
        query_copy(d).wait_recv()

    @pl.loop(0, NX)
    def _(at):
        attend(at)

    @pl.loop(1, last)
    def _(i):
        arrive(i)
        project(i)

        @pl.loop(0, NX)
        def _(at):
            attend(at)

    arrive(last)
    project(last)

    def chip_at(i):
        return lax.rem(x + 2 + lax.div(i * (i + 1), 2), NX)

    def pair_copy(i):
        return pltpu.make_async_remote_copy(
            src_ref=pair_out.at[i],
            dst_ref=pair_in.at[i],
            send_sem=psend_sem.at[i],
            recv_sem=precv_sem.at[i],
            device_id={"ctx": 2 * x + 1 - core},
            device_id_type=MESH,
        )

    half_width = width // 2

    def cross_copy(kind, way):
        return pltpu.make_async_remote_copy(
            src_ref=cross_out.at[kind, way],
            dst_ref=cross_in.at[kind, way],
            send_sem=xsend_sem.at[kind, way],
            recv_sem=xrecv_sem.at[kind, way],
            device_id={"ctx": 2 * lax.rem(x + (1 if way == 0 else NX - 1), NX) + core},
            device_id_type=MESH,
        )

    def columns(k):
        return slice(k * half_width, (k + 1) * half_width)

    def part_of(i, which):
        at = 2 * chip_at(i) + which
        return acc[pl.ds(pl.multiple_of(at * cands, cands), cands), :]

    def summed(i):
        pair_copy(i).wait_recv()
        return part_of(i, core) + pair_in[i].astype(jnp.float32)

    def hand_on():
        both = summed(0).astype(jnp.bfloat16)
        for way in (0, 1):
            cross_out[0, way] = both[:, columns(way)]
            cross_copy(0, way).start()

    def direct(i, way):
        own[way] = summed(i)
        cross_out[2, way] = own[way][:, columns(1 - way)].astype(jnp.bfloat16)
        cross_copy(2, way).start()

    def relay(way):
        cross_copy(0, way).wait_recv()
        cross_out[1, way] = (
            own[way][:, columns(way)] + cross_in[0, way].astype(jnp.float32)
        ).astype(jnp.bfloat16)
        cross_copy(1, way).start()

    @pl.loop(0, NX)
    def _(i):
        attend(chip_at(i))
        pair_out[i] = part_of(i, 1 - core).astype(jnp.bfloat16)
        pair_copy(i).start()

        @pl.when(i == 1)
        def _():
            hand_on()

        @pl.when(i == 2)
        def _():
            direct(1, 1)

        @pl.when(i == 3)
        def _():
            direct(2, 0)

    relay(1)
    relay(0)
    total = summed(NX - 1)
    loads[5].wait()
    for kind in (2, 1):
        for way in (0, 1):
            cross_copy(kind, way).wait_recv()
    sides = [
        cross_in[1, way].astype(jnp.float32) + cross_in[2, 1 - way].astype(jnp.float32)
        for way in (0, 1)
    ]
    attended = total + jnp.concatenate(sides, axis=1)
    mean = jnp.mean(attended, axis=-1, keepdims=True)
    centred = attended - mean
    variance = jnp.mean(centred * centred, axis=-1, keepdims=True)
    mixed = (centred * lax.rsqrt(variance + 1e-05) * gate[...]).astype(jnp.bfloat16)
    result = cand[...].astype(jnp.float32) + jnp.dot(
        mixed, wout[...], preferred_element_type=jnp.float32
    )
    out_ref[...] = result.astype(jnp.bfloat16)

    for j in range(1, NY):
        exchange(0, j).wait_send()

    @pl.loop(1, NZ)
    def _(i):
        for j in range(NY):
            exchange(i, j).wait_send()

    for d in range(1, 2 * NX):
        query_copy(d).wait_send()
    for i in range(NX):
        pair_copy(i).wait_send()
    for kind in range(3):
        for way in (0, 1):
            cross_copy(kind, way).wait_send()


def on_device(history, block_owner, candidates, w_kv, w_qu, w_out):
    rows, width = history.shape
    blocks = block_owner.shape[0]
    events = rows // blocks
    cands = candidates.shape[0]
    group = NY * CAP * events
    total = NZ * group
    count = NY * NZ
    bf16, f32 = jnp.bfloat16, jnp.float32
    dma = pltpu.SemaphoreType.DMA
    anywhere = pl.BlockSpec(memory_space=pl.ANY)
    vmem = pl.BlockSpec(memory_space=pltpu.VMEM)
    return pl.pallas_call(
        layer_kernel,
        out_shape=jax.ShapeDtypeStruct((cands, width), bf16),
        in_specs=[anywhere] * 6,
        out_specs=vmem,
        scratch_shapes=[
            pltpu.VMEM((1, blocks), jnp.int32),
            pltpu.VMEM((rows, width), bf16),
            pltpu.VMEM((cands, width), bf16),
            pltpu.VMEM((width, 2 * width), bf16),
            pltpu.VMEM((width, 2 * width), bf16),
            pltpu.VMEM((width, width), bf16),
            pltpu.VMEM((total, width), bf16),
            pltpu.VMEM((total, width), bf16),
            pltpu.VMEM((2 * NX * cands, width), bf16),
            pltpu.VMEM((cands, width), f32),
            pltpu.VMEM((group, width), bf16),
            pltpu.VMEM((group, width), bf16),
            pltpu.VMEM((2 * NX * cands, width), f32),
            pltpu.VMEM((NX, cands, width), bf16),
            pltpu.VMEM((NX, cands, width), bf16),
            pltpu.VMEM((3, 2, cands, width // 2), bf16),
            pltpu.VMEM((3, 2, cands, width // 2), bf16),
            pltpu.VMEM((2, cands, width), f32),
            dma((6,)),
            dma((count,)),
            dma((count,)),
            dma((2 * NX,)),
            dma((2 * NX,)),
            dma((NX,)),
            dma((NX,)),
            dma((3, 2)),
            dma((3, 2)),
        ],
        compiler_params=pltpu.CompilerParams(
            collective_id=0, has_side_effects=True, vmem_limit_bytes=60 * 2**20
        ),
    )(block_owner.reshape(1, blocks), history, candidates, w_kv, w_qu, w_out)


def solution(mesh):
    in_specs = (P(REQ_CTX, None), P(REQ_CTX, None), P(REQ_CTX, None), P(), P(), P())
    return jax.shard_map(
        on_device, mesh=mesh, in_specs=in_specs, out_specs=P(REQ_CTX, None), check_vma=False
    )
```

```python
import functools

import jax
import jax.numpy as jnp
from jax import lax
from jax.experimental import pallas as pl
from jax.experimental.pallas import tpu as pltpu
from jax.sharding import PartitionSpec as P

HEAD = 128
REQ_CTX = ("req", "ctx")
NY, NZ, NX = 4, 8, 4
CAP = 3
MESH = pl.DeviceIdType.MESH


def silu(v):
    half = 0.5 * v
    return half + half * jnp.tanh(half)


def chunk_dz(i):
    return lax.rem(NZ + lax.div(i + 1, 2) * (2 * lax.rem(i, 2) - 1), NZ)


def layer_kernel(
    owner_ref, hist_ref, cand_ref, wkv_ref, wqu_ref, wout_ref, out_ref,
    owners, hist, cand, wkv, wqu, wout,
    send, recv, queries, gate, keys, values, acc,
    pair_out, pair_in, cross_out, cross_in, own,
    load_sem, send_sem, recv_sem, qsend_sem, qrecv_sem,
    psend_sem, precv_sem, xsend_sem, xrecv_sem,
):
    req, ctx = lax.axis_index("req"), lax.axis_index("ctx")
    y, z = lax.div(req, NZ), lax.rem(req, NZ)
    x, core = lax.div(ctx, 2), lax.rem(ctx, 2)
    rows, width = hist.shape
    blocks = owner_ref.shape[1]
    events = rows // blocks
    unit = CAP * events
    group = NY * unit
    cands = cand.shape[0]
    heads = width // HEAD

    loads = []
    for k, (src, dst) in enumerate(
        (
            (owner_ref, owners), (hist_ref, hist), (cand_ref, cand),
            (wqu_ref, wqu), (wkv_ref, wkv), (wout_ref, wout),
        )
    ):
        copy = pltpu.make_async_copy(src, dst, load_sem.at[k])
        copy.start()
        loads.append(copy)

    barrier = pltpu.get_barrier_semaphore()
    for d in range(1, NY * NZ):
        pl.semaphore_signal(
            barrier, inc=1, device_id={"req": lax.rem(req + d, NY * NZ)}, device_id_type=MESH
        )
    for d in range(1, 2 * NX):
        pl.semaphore_signal(
            barrier, inc=1, device_id={"ctx": lax.rem(ctx + d, 2 * NX)}, device_id_type=MESH
        )

    loads[0].wait()
    spot = lax.broadcasted_iota(jnp.int32, (blocks, blocks), 0)
    diagonal = spot == lax.broadcasted_iota(jnp.int32, (blocks, blocks), 1)
    listed = owners[...].astype(jnp.float32)
    owner = jnp.sum(jnp.where(diagonal, listed, 0.0), axis=1, keepdims=True)
    block_of = lax.div(lax.broadcasted_iota(jnp.int32, (blocks, rows), 1), events)
    earlier = lax.broadcasted_iota(jnp.int32, (blocks, rows), 0)
    owner_row = jnp.sum(jnp.where(earlier == block_of, owner, 0.0), axis=0, keepdims=True)
    same = jnp.logical_and(owner == owner_row, earlier < block_of)
    rank = jnp.sum(jnp.where(same, 1.0, 0.0), axis=0, keepdims=True)
    event = lax.rem(lax.broadcasted_iota(jnp.int32, (1, rows), 1), events)
    place = owner_row.astype(jnp.int32) * unit + rank.astype(jnp.int32) * events + event

    loads[1].wait()

    def exchange(i, j):
        to_y = lax.rem(y + j, NY)
        to_z = lax.rem(z + chunk_dz(i), NZ)
        spot = i * NY + j
        return pltpu.make_async_remote_copy(
            src_ref=send.at[pl.ds(pl.multiple_of(spot * unit, unit), unit)],
            dst_ref=recv.at[pl.ds(pl.multiple_of(spot * unit, unit), unit)],
            send_sem=send_sem.at[spot],
            recv_sem=recv_sem.at[spot],
            device_id={"req": to_y * NZ + to_z},
            device_id_type=MESH,
        )

    line = lax.broadcasted_iota(jnp.int32, (group, 1), 0)
    turn = sum(jnp.where(line >= unit * k, 1, 0) for k in range(1, NY))
    inside = line - turn * unit

    def pack(i):
        to_z = lax.rem(z + chunk_dz(i), NZ)
        target = (lax.rem(y + turn, NY) * NZ + to_z) * unit + inside
        placing = jnp.where(target == place, 1.0, 0.0).astype(jnp.bfloat16)
        return jnp.dot(placing, hist[...], preferred_element_type=jnp.float32).astype(jnp.bfloat16)

    last, early = NZ - 1, 3
    made = pack(0)
    recv[:unit, :] = made[:unit]
    send[unit:group, :] = made[unit:]

    @pl.loop(1, early)
    def _(i):
        send[pl.ds(pl.multiple_of(i * group, group), group), :] = pack(i)

    pl.semaphore_wait(barrier, NY * NZ + 2 * NX - 2)
    for i in range(1, early):
        for j in range(NY):
            exchange(i, j).start()
    for j in range(1, NY):
        exchange(0, j).start()

    loads[2].wait()
    loads[3].wait()
    mine = pl.ds(pl.multiple_of(ctx * cands, cands), cands)
    queries[mine, :] = silu(
        jnp.dot(cand[...], wqu[:, :width], preferred_element_type=jnp.float32)
    ).astype(jnp.bfloat16)

    def query_copy(d):
        return pltpu.make_async_remote_copy(
            src_ref=queries.at[mine],
            dst_ref=queries.at[mine],
            send_sem=qsend_sem.at[d],
            recv_sem=qrecv_sem.at[d],
            device_id={"ctx": lax.rem(ctx + d, 2 * NX)},
            device_id_type=MESH,
        )

    for d in range(1, 2 * NX):
        query_copy(d).start()

    @pl.loop(early, NZ)
    def _(i):
        send[pl.ds(pl.multiple_of(i * group, group), group), :] = pack(i)
        for j in range(NY):
            exchange(i, j).start()

    gate[...] = silu(jnp.dot(cand[...], wqu[:, width:], preferred_element_type=jnp.float32))
    acc[...] = jnp.zeros_like(acc)
    loads[4].wait()

    def arrive(i):
        for j in range(NY):
            exchange(i, j).wait_recv()

    def project(i):
        events_in = recv[pl.ds(pl.multiple_of(i * group, group), group), :]
        keys[...] = silu(
            jnp.dot(events_in, wkv[:, :width], preferred_element_type=jnp.float32)
        ).astype(jnp.bfloat16)
        values[...] = jnp.dot(
            events_in, wkv[:, width:], preferred_element_type=jnp.float32
        ).astype(jnp.bfloat16)

    span = 2 * cands
    factor = 0.5 * HEAD ** (-0.5)

    def attend(at):
        here = pl.ds(pl.multiple_of(at * span, span), span)
        for h in range(heads):
            cols = slice(h * HEAD, (h + 1) * HEAD)
            scores = lax.dot_general(
                queries[here, cols], keys[:, cols], (((1,), (1,)), ((), ())),
                preferred_element_type=jnp.float32,
            )
            half = scores * factor
            weight = (half + half * jnp.tanh(half)).astype(jnp.bfloat16)
            acc[here, cols] += jnp.dot(
                weight, values[:, cols], preferred_element_type=jnp.float32
            )

    for j in range(1, NY):
        exchange(0, j).wait_recv()
    project(0)
    for d in range(1, 2 * NX):
        query_copy(d).wait_recv()

    @pl.loop(0, NX)
    def _(at):
        attend(at)

    @pl.loop(1, last)
    def _(i):
        arrive(i)
        project(i)

        @pl.loop(0, NX)
        def _(at):
            attend(at)

    arrive(last)
    project(last)

    def chip_at(i):
        return lax.rem(x + 2 + lax.div(i * (i + 1), 2), NX)

    def pair_copy(i):
        return pltpu.make_async_remote_copy(
            src_ref=pair_out.at[i],
            dst_ref=pair_in.at[i],
            send_sem=psend_sem.at[i],
            recv_sem=precv_sem.at[i],
            device_id={"ctx": 2 * x + 1 - core},
            device_id_type=MESH,
        )

    half_width = width // 2

    def cross_copy(kind, way):
        return pltpu.make_async_remote_copy(
            src_ref=cross_out.at[kind, way],
            dst_ref=cross_in.at[kind, way],
            send_sem=xsend_sem.at[kind, way],
            recv_sem=xrecv_sem.at[kind, way],
            device_id={"ctx": 2 * lax.rem(x + (1 if way == 0 else NX - 1), NX) + core},
            device_id_type=MESH,
        )

    def columns(k):
        return slice(k * half_width, (k + 1) * half_width)

    def part_of(i, which):
        at = 2 * chip_at(i) + which
        return acc[pl.ds(pl.multiple_of(at * cands, cands), cands), :]

    def summed(i):
        pair_copy(i).wait_recv()
        return part_of(i, core) + pair_in[i].astype(jnp.float32)

    def hand_on():
        both = summed(0).astype(jnp.bfloat16)
        for way in (0, 1):
            cross_out[0, way] = both[:, columns(way)]
            cross_copy(0, way).start()

    def direct(i, way):
        own[way] = summed(i)
        cross_out[2, way] = own[way][:, columns(1 - way)].astype(jnp.bfloat16)
        cross_copy(2, way).start()

    def relay(way):
        cross_copy(0, way).wait_recv()
        cross_out[1, way] = (
            own[way][:, columns(way)] + cross_in[0, way].astype(jnp.float32)
        ).astype(jnp.bfloat16)
        cross_copy(1, way).start()

    @pl.loop(0, NX)
    def _(i):
        attend(chip_at(i))
        pair_out[i] = part_of(i, 1 - core).astype(jnp.bfloat16)
        pair_copy(i).start()

        @pl.when(i == 1)
        def _():
            hand_on()

        @pl.when(i == 2)
        def _():
            direct(1, 1)

        @pl.when(i == 3)
        def _():
            direct(2, 0)

    relay(1)
    relay(0)
    total = summed(NX - 1)
    loads[5].wait()
    for kind in (2, 1):
        for way in (0, 1):
            cross_copy(kind, way).wait_recv()
    sides = [
        cross_in[1, way].astype(jnp.float32) + cross_in[2, 1 - way].astype(jnp.float32)
        for way in (0, 1)
    ]
    attended = total + jnp.concatenate(sides, axis=1)
    mean = jnp.mean(attended, axis=-1, keepdims=True)
    centred = attended - mean
    variance = jnp.mean(centred * centred, axis=-1, keepdims=True)
    mixed = (centred * lax.rsqrt(variance + 1e-05) * gate[...]).astype(jnp.bfloat16)
    result = cand[...].astype(jnp.float32) + jnp.dot(
        mixed, wout[...], preferred_element_type=jnp.float32
    )
    out_ref[...] = result.astype(jnp.bfloat16)

    for j in range(1, NY):
        exchange(0, j).wait_send()

    @pl.loop(1, NZ)
    def _(i):
        for j in range(NY):
            exchange(i, j).wait_send()

    for d in range(1, 2 * NX):
        query_copy(d).wait_send()
    for i in range(NX):
        pair_copy(i).wait_send()
    for kind in range(3):
        for way in (0, 1):
            cross_copy(kind, way).wait_send()


def on_device(history, block_owner, candidates, w_kv, w_qu, w_out):
    rows, width = history.shape
    blocks = block_owner.shape[0]
    events = rows // blocks
    cands = candidates.shape[0]
    group = NY * CAP * events
    total = NZ * group
    count = NY * NZ
    bf16, f32 = jnp.bfloat16, jnp.float32
    dma = pltpu.SemaphoreType.DMA
    anywhere = pl.BlockSpec(memory_space=pl.ANY)
    vmem = pl.BlockSpec(memory_space=pltpu.VMEM)
    return pl.pallas_call(
        layer_kernel,
        out_shape=jax.ShapeDtypeStruct((cands, width), bf16),
        in_specs=[anywhere] * 6,
        out_specs=vmem,
        scratch_shapes=[
            pltpu.VMEM((1, blocks), jnp.int32),
            pltpu.VMEM((rows, width), bf16),
            pltpu.VMEM((cands, width), bf16),
            pltpu.VMEM((width, 2 * width), bf16),
            pltpu.VMEM((width, 2 * width), bf16),
            pltpu.VMEM((width, width), bf16),
            pltpu.VMEM((total, width), bf16),
            pltpu.VMEM((total, width), bf16),
            pltpu.VMEM((2 * NX * cands, width), bf16),
            pltpu.VMEM((cands, width), f32),
            pltpu.VMEM((group, width), bf16),
            pltpu.VMEM((group, width), bf16),
            pltpu.VMEM((2 * NX * cands, width), f32),
            pltpu.VMEM((NX, cands, width), bf16),
            pltpu.VMEM((NX, cands, width), bf16),
            pltpu.VMEM((3, 2, cands, width // 2), bf16),
            pltpu.VMEM((3, 2, cands, width // 2), bf16),
            pltpu.VMEM((2, cands, width), f32),
            dma((6,)),
            dma((count,)),
            dma((count,)),
            dma((2 * NX,)),
            dma((2 * NX,)),
            dma((NX,)),
            dma((NX,)),
            dma((3, 2)),
            dma((3, 2)),
        ],
        compiler_params=pltpu.CompilerParams(
            collective_id=0, has_side_effects=True, vmem_limit_bytes=60 * 2**20
        ),
    )(block_owner.reshape(1, blocks), history, candidates, w_kv, w_qu, w_out)


def solution(mesh):
    in_specs = (P(REQ_CTX, None), P(REQ_CTX, None), P(REQ_CTX, None), P(), P(), P())
    return jax.shard_map(
        on_device, mesh=mesh, in_specs=in_specs, out_specs=P(REQ_CTX, None), check_vma=False
    )
```
